32 devices in a mesh: wide: 16 (over z, y, x), narrow: 2 (over core).
Axes of the slice: x: 2, y: 2, z: 4, core: 2. Of those that a mesh axis runs over, the one named last changes fastest.
Arguments:
- tokens: bfloat16 [2048, 2048], P('wide'), may hold values from -6 to 6
- expert_ids: int32 [2048, 6], P('wide'), may hold values from 0 to 15, all different within a row; in each aligned block of 128 rows (0 to 127, 128 to 255, ...) at most 64 rows name the same one
- gate_weights: float32 [2048, 6], P('wide'), may hold values from 0.05 to 0.6
- shared_gate: bfloat16 [2048, 2816], P('wide', 'narrow'), may hold values from -0.125 to 0.125
- shared_up: bfloat16 [2048, 2816], P('wide', 'narrow'), may hold values from -0.125 to 0.125
- shared_down: bfloat16 [2816, 2048], P('narrow', 'wide'), may hold values from -0.109375 to 0.109375
- expert_gate: bfloat16 [16, 2048, 1408], P('wide', None, 'narrow'), may hold values from -0.125 to 0.125
- expert_up: bfloat16 [16, 2048, 1408], P('wide', None, 'narrow'), may hold values from -0.125 to 0.125
- expert_down: bfloat16 [16, 1408, 2048], P('wide', 'narrow'), may hold values from -0.15625 to 0.15625
Outputs:
- moe_out: bfloat16 [2048, 2048], P('wide', 'narrow')
The draws below stay inside these ranges and needn't reach their ends.
Inputs may be any that keep to these rules, and one draw needn't show every extreme that they name: `expert_ids`: the 6 ids of a row differ. Among the 128 rows of one index of wide, no expert is named by more than 64 rows.
All inputs are finite; a program needn't handle non-finite values.
Results may differ from the reference program's by a relative error of at most 0.0075.
Values may be sent and summed in bfloat16 or wider, within the bound.
A program may use at most 128 MiB of HBM per device.

```python
import math
import jax
import jax.numpy as jnp
import numpy as np
from jax import lax

D = 2048
MF = 1408
FS = 2816
TOP = 6
TOK_DEV = 128
EXPERTS = 16
TOKENS = 2048
CAP = 64
N_WIDE = 16
N_NARROW = 2


def block_scale(stream_key, dims, split, low, high):
    def one(axis_at, blocks):
        steps = jax.random.uniform(jax.random.fold_in(jax.random.fold_in(stream_key, 6), axis_at), (blocks,), jnp.float32, low / len(split), high / len(split))
        return jnp.repeat(jnp.exp(steps), dims[axis_at] // blocks).reshape((-1,) + (1,) * (len(dims) - axis_at - 1))

    factor_of = one(*split[0])
    for cut in split[1:]:
        factor_of = factor_of * one(*cut)
    return factor_of


def shared_out(rng, own, number, rows, number_of, top, most, slope):
    ranking = jax.random.permutation(rng, number_of)
    packed, usual = load_shares(number_of, rows * top, most, slope, True), load_shares(number_of, rows * top, most, slope, False)
    places = jnp.arange(number_of)

    def named(lengths, offset_by):
        used = int((lengths > 0).sum())
        fixed = max(1, used // 4)
        passed = fixed + (places - fixed + offset_by * (used - fixed)) % max(1, number_of - fixed)
        return jnp.zeros((number_of,), jnp.int32).at[ranking[jnp.where(places < fixed, places, passed)]].set(jnp.asarray(lengths, jnp.int32))

    lengths = jnp.where(number % 4 == 0, named(packed, number // 4), named(usual, number - number // 4 - 1))
    mixed = jax.random.permutation(jax.random.fold_in(own, 3), number_of)
    donor, receiver = mixed[0:number_of // 2 * 2:2], mixed[1:number_of // 2 * 2:2]
    margin = jnp.minimum(lengths[donor] - 1, most - lengths[receiver]) // 2
    margin = jnp.where((donor == ranking[0]) | (receiver == ranking[0]) | (lengths[receiver] == 0), 0, jnp.maximum(margin, 0))
    passed = jax.random.randint(jax.random.fold_in(own, 4), (number_of // 2,), 0, 1 << 20) % (margin + 1)
    lengths = lengths.at[donor].add(-passed).at[receiver].add(passed)
    labels = jnp.searchsorted(jnp.cumsum(lengths), jnp.arange(rows * top), side="right").astype(jnp.int32)
    listing = labels.reshape(top, rows).T
    listing = listing[jax.random.permutation(jax.random.fold_in(own, 1), rows)]
    offset_by = jax.random.randint(jax.random.fold_in(own, 2), (rows, 1), 0, top)
    return jnp.take_along_axis(listing, (jnp.arange(top)[None, :] + offset_by) % top, axis=1)


def load_shares(amount, total, limit, lean, full):
    portions = [(1 << 20) // math.isqrt(grade ** lean) + 1 for grade in range(1, amount + 1)]
    largest = limit if full else min(limit, max(-(-total // amount), total * portions[0] // sum(portions)))
    least = 1 if total - largest >= amount - 1 else 0
    counts, surplus = [largest] + [least] * (amount - 1), total - largest - least * (amount - 1)
    while surplus > 0:
        candidates = [i for i in range(1, amount) if counts[i] < largest] or [i for i in range(1, amount) if counts[i] < limit]
        whole, budget = sum([portions[i] for i in candidates]), surplus
        for i in candidates:
            more = min(limit - counts[i], max(1, budget * portions[i] // whole), surplus)
            counts[i] = counts[i] + more
            surplus = surplus - more
    return np.array(counts)


def normal_values(stream_key, extent, spread, reach, cuts=(), held_as=jnp.bfloat16):
    array = jax.random.normal(stream_key, extent, jnp.float32) * spread
    if len(cuts) > 0:
        array = block_scale(stream_key, extent, cuts, -0.22, 0.18) * array
    return jnp.clip(array, min=-reach, max=reach).astype(held_as)


def setup_inputs(seed: int = 0) -> dict:
    keys = jax.random.split(jax.random.key(seed), 10)
    tokens = normal_values(keys[0], (TOKENS, D), 1.0, 6.0, ((0, 16),))
    expert_ids_keys = jax.random.split(jax.random.fold_in(keys[1], 1), TOKENS // TOK_DEV)
    expert_ids_turns = jax.random.permutation(jax.random.fold_in(keys[1], 3), TOKENS // TOK_DEV)
    expert_ids = jax.vmap(lambda own, number: shared_out(jax.random.fold_in(keys[1], 2), own, number, TOK_DEV, EXPERTS, TOP, CAP, 2))(expert_ids_keys, expert_ids_turns).reshape((TOKENS, TOP))
    gate_weights = jnp.clip(jnp.exp(math.log(0.6) - 2.4849067 * jax.random.uniform(keys[2], (TOKENS, TOP), jnp.float32) ** block_scale(keys[2], (TOKENS, TOP), ((0, 16),), -0.2, 0.2)), 0.05, 0.6)
    shared_gate = normal_values(keys[3], (D, FS), D ** -0.5, 0.125, ((0, 16), (1, 2)))
    shared_up = normal_values(keys[4], (D, FS), D ** -0.5, 0.125, ((0, 16), (1, 2)))
    shared_down = normal_values(keys[5], (FS, D), FS ** -0.5, 0.109375, ((0, 2), (1, 16)))
    expert_gate = normal_values(keys[6], (EXPERTS, D, MF), D ** -0.5, 0.125, ((0, 16), (2, 2)))
    expert_up = normal_values(keys[7], (EXPERTS, D, MF), D ** -0.5, 0.125, ((0, 16), (2, 2)))
    expert_down = normal_values(keys[8], (EXPERTS, MF, D), MF ** -0.5, 0.15625, ((0, 16), (1, 2)))
    return {"tokens": tokens, "expert_ids": expert_ids, "gate_weights": gate_weights, "shared_gate": shared_gate, "shared_up": shared_up, "shared_down": shared_down, "expert_gate": expert_gate, "expert_up": expert_up, "expert_down": expert_down}


def expert_rows(rows_in, w_gate, w_up, w_down):
    gate_part = jnp.dot(rows_in, w_gate, preferred_element_type=jnp.float32)
    up_part = jnp.dot(rows_in, w_up, preferred_element_type=jnp.float32)
    hidden = (jax.nn.silu(gate_part) * up_part).astype(jnp.bfloat16)
    quarter = MF // N_NARROW
    summed = jnp.zeros((rows_in.shape[0], w_down.shape[1]), jnp.float32)
    for slice_idx in range(N_NARROW):
        lower = slice_idx * quarter
        partial_value = jnp.dot(hidden[:, lower:lower + quarter], w_down[lower:lower + quarter], preferred_element_type=jnp.float32)
        summed = summed + partial_value.astype(jnp.bfloat16).astype(jnp.float32)
    return summed.astype(jnp.bfloat16)


def reference(tokens, expert_ids, gate_weights, shared_gate, shared_up, shared_down, expert_gate, expert_up, expert_down):
    shared_g = jnp.dot(tokens, shared_gate, preferred_element_type=jnp.float32)
    shared_u = jnp.dot(tokens, shared_up, preferred_element_type=jnp.float32)
    shared_hidden = (jax.nn.silu(shared_g) * shared_u).astype(jnp.bfloat16)
    shared = jnp.dot(shared_hidden, shared_down, preferred_element_type=jnp.float32)
    slot_count = N_WIDE * CAP
    positions = jnp.arange(TOKENS, dtype=jnp.int32)

    def one_expert(routed, inputs):
        expert_index, w_gate, w_up, w_down = inputs
        matches = expert_ids == expert_index
        chosen = jnp.any(matches, axis=1)
        weight = jnp.sum(jnp.where(matches, gate_weights, jnp.float32(0.0)), axis=1)
        rank_pos = (jnp.cumsum(chosen.astype(jnp.int32)) - 1).astype(jnp.int32)
        target = jnp.where(chosen, rank_pos, slot_count).astype(jnp.int32)
        picked = jnp.zeros((slot_count + 1,), jnp.int32).at[target].set(positions)[:slot_count]
        weight_live = jnp.zeros((slot_count + 1,), jnp.float32).at[target].set(weight)[:slot_count]
        outputs = expert_rows(tokens[picked], w_gate, w_up, w_down)
        routed = routed.at[picked].add(weight_live[:, None] * outputs.astype(jnp.float32))
        return routed, None

    routed0 = jnp.zeros((TOKENS, D), jnp.float32)
    indices = jnp.arange(EXPERTS, dtype=jnp.int32)
    routed, unused = lax.scan(one_expert, routed0, (indices, expert_gate, expert_up, expert_down))
    return (shared + routed).astype(jnp.bfloat16)
```

```python
import functools

import jax
import jax.numpy as jnp
from jax import lax
from jax.experimental import pallas as pl
from jax.experimental.pallas import tpu as pltpu
from jax.sharding import PartitionSpec as P


def expert_ffn(received, w_gate, w_up, w_down):
    senders, items, width = received.shape
    flat_rows = received.reshape(senders * items, width)
    gate_part = jnp.dot(flat_rows, w_gate, preferred_element_type=jnp.float32)
    up_part = jnp.dot(flat_rows, w_up, preferred_element_type=jnp.float32)
    hidden = (jax.nn.silu(gate_part) * up_part).astype(jnp.bfloat16)
    partial_value = jnp.dot(hidden, w_down, preferred_element_type=jnp.float32).astype(jnp.bfloat16)
    return partial_value.reshape(senders, items, w_down.shape[1])


def dispatch_body(
    tokens,
    expert_ids,
    gate_weights,
    shared_gate,
    shared_up,
    shared_down,
    expert_gate,
    expert_up,
    expert_down,
):
    tok_count, width = tokens.shape
    top_count = expert_ids.shape[1]
    experts = lax.axis_size("wide") * expert_gate.shape[0]
    capacity = min(tok_count, 4 * tok_count * top_count // (3 * experts))
    narrow_count = lax.axis_size("narrow")
    w_gate = expert_gate[0]
    w_up = expert_up[0]
    w_down = expert_down[0]
    pairs = tok_count * top_count
    flat_ids = expert_ids.reshape(pairs)
    onehot = (flat_ids[:, None] == jnp.arange(experts, dtype=jnp.int32)[None, :]).astype(jnp.int32)
    before = jnp.cumsum(onehot, axis=0) - onehot
    slot_pos = jnp.sum(before * onehot, axis=1)
    target_slot = flat_ids * capacity + slot_pos
    source = (
        jnp.full((experts * capacity,), -1, jnp.int32)
        .at[target_slot]
        .set(jnp.arange(pairs, dtype=jnp.int32))
    )
    filled = source >= 0
    token_of = jnp.where(filled, source // top_count, 0)
    outgoing = jnp.where(filled[:, None], tokens[token_of], jnp.zeros((), jnp.bfloat16))
    outgoing = outgoing.reshape(experts, capacity, width)
    quarter = capacity // narrow_count
    own_rows = lax.dynamic_slice_in_dim(outgoing, lax.axis_index("narrow") * quarter, quarter, 1)
    arrived = lax.all_to_all(own_rows, "wide", split_axis=0, concat_axis=0, tiled=True)
    joined = lax.all_gather(arrived, "narrow", axis=1, tiled=True)
    partial_value = expert_ffn(joined, w_gate, w_up, w_down)
    expert_out = (
        lax.psum_scatter(partial_value, "narrow", scatter_dimension=2, tiled=True)
        .astype(jnp.float32)
        .astype(jnp.bfloat16)
    )
    returned = lax.all_to_all(expert_out, "wide", split_axis=0, concat_axis=0, tiled=True)
    returned_rows = returned.reshape(experts * capacity, returned.shape[2])
    pair_rows = returned_rows[target_slot].astype(jnp.float32)
    weighted = gate_weights.reshape(pairs, 1) * pair_rows
    routed = jnp.sum(weighted.reshape(tok_count, top_count, returned.shape[2]), axis=1)
    gate_sum = jnp.dot(
        tokens,
        lax.all_gather(shared_gate, "wide", axis=0, tiled=True),
        preferred_element_type=jnp.float32,
    )
    up_sum = jnp.dot(
        tokens,
        lax.all_gather(shared_up, "wide", axis=0, tiled=True),
        preferred_element_type=jnp.float32,
    )
    shared_hidden = (jax.nn.silu(gate_sum) * up_sum).astype(jnp.bfloat16)
    shared_terms = jnp.dot(
        shared_hidden,
        lax.all_gather(shared_down, "wide", axis=1, tiled=True),
        preferred_element_type=jnp.float32,
    )
    shared = lax.psum_scatter(shared_terms, "narrow", scatter_dimension=1, tiled=True)
    return (shared + routed).astype(jnp.bfloat16)


MESH = pl.DeviceIdType.MESH
ANY = pl.BlockSpec(memory_space=pl.ANY)
VMEM = pl.BlockSpec(memory_space=pltpu.VMEM)
LANES = 128
PLANE = 4


def plan(tok_count, top_count, experts, wide_count):
    capacity = min(tok_count, 4 * tok_count * top_count // (3 * experts))
    return capacity, wide_count * tok_count <= 4 * experts * capacity


def greet(devices):
    barrier = pltpu.get_barrier_semaphore()
    for device in devices:
        pl.semaphore_signal(barrier, inc=1, device_id=device, device_id_type=MESH)
    pl.semaphore_wait(barrier, len(devices))


def gather_kernel(
    wide, tok, gate, up, down, dense, every, all_gate, all_up, all_down, weight, send, recv, local
):
    me = lax.axis_index("wide")
    core = lax.axis_index("narrow")
    lines = wide // PLANE
    count = tok.shape[0]
    rows = count // 2
    half = rows // 2
    pieces = gate.shape[1] // LANES
    greet([(me ^ k, core) for k in range(1, wide)] + [(me, 1 - core)])

    def region(chip, side=None):
        start = chip * count + core * rows
        if side is None:
            return every.at[pl.ds(pl.multiple_of(start, rows), rows)]
        return every.at[pl.ds(pl.multiple_of(start + side * half, half), half)]

    def copy(number, source, target, device):
        return pltpu.make_async_remote_copy(
            src_ref=source,
            dst_ref=target,
            send_sem=send.at[number],
            recv_sem=recv.at[number],
            device_id=device,
            device_id_type=MESH,
        )

    x_peer, y_peer, twin = (me ^ 1, core), (me ^ 2, core), (me, 1 - core)
    Z, X, Y = 0, lines, 2 * lines
    XD, YD, T = 3 * lines, 4 * lines, 5 * lines
    W = T + 5 * lines
    started = []

    def start(item):
        item.start()
        started.append(item)

    def arrive(number, place):
        copy(number, place, place, twin).wait_recv()
        start(copy(T + number, place, place, twin))

    own = pltpu.make_async_copy(
        tok, every.at[pl.ds(pl.multiple_of(me * count, count), count)], local.at[0]
    )
    own.start()
    mine = tok.at[pl.ds(pl.multiple_of(core * rows, rows), rows)]
    start(copy(X, mine, region(me), x_peer))
    start(copy(Y, mine, region(me), y_peer))
    for d in range(1, lines):
        start(copy(Z + d, mine, region(me), (me ^ (PLANE * d), core)))
    dense_copies = []
    for k in range(1, wide):
        item = copy(W + k, dense.at[me ^ k], weight.at[me], (me ^ k, core))
        item.start()
        dense_copies.append(item)
    dense_own = pltpu.make_async_copy(dense.at[me], weight.at[me], local.at[1])
    dense_own.start()

    def line(d):
        chip = me ^ (PLANE * d)
        arrive(Z + d, region(chip))
        start(copy(X + d, region(chip), region(chip), x_peer))
        start(copy(Y + d, region(chip), region(chip), y_peer))

    def beside(d):
        chip = me ^ 1 ^ (PLANE * d)
        arrive(X + d, region(chip))
        start(copy(YD + d, region(chip, 1), region(chip, 1), y_peer))
        chip = me ^ 2 ^ (PLANE * d)
        arrive(Y + d, region(chip))
        start(copy(XD + d, region(chip, 0), region(chip, 0), x_peer))

    def shared_copies(k):
        to = me ^ k
        part = pl.ds(pl.multiple_of(to * LANES, LANES), LANES)
        place = pl.ds(pl.multiple_of(me * LANES, LANES), LANES)
        base = W + k
        return [
            copy(base + wide, gate.at[:, part], all_gate.at[place], (to, core)),
            copy(base + 2 * wide, up.at[:, part], all_up.at[place], (to, core)),
            copy(base + 3 * wide, down.at[part], all_down.at[:, place], (to, core)),
        ]

    beside(0)
    for d in range(1, lines):
        line(d)
        if d >= 2:
            beside(d - 1)

    for k in range(1, wide):

        @pl.when((me ^ k) < pieces)
        def _():
            for item in shared_copies(k):
                item.start()

    @pl.when(me < pieces)
    def _():
        part = pl.ds(pl.multiple_of(me * LANES, LANES), LANES)
        items = [
            pltpu.make_async_copy(gate.at[:, part], all_gate.at[part], local.at[2]),
            pltpu.make_async_copy(up.at[:, part], all_up.at[part], local.at[3]),
            pltpu.make_async_copy(down.at[part], all_down.at[:, part], local.at[4]),
        ]
        for item in items:
            item.start()
        for item in items:
            item.wait()

    @pl.when(me >= pieces)
    def _():
        all_gate[...] = jnp.zeros_like(all_gate)
        all_up[...] = jnp.zeros_like(all_up)
        all_down[...] = jnp.zeros_like(all_down)

    beside(lines - 1)
    for d in range(lines):
        arrive(XD + d, region(me ^ 3 ^ (PLANE * d), 0))
        arrive(YD + d, region(me ^ 3 ^ (PLANE * d), 1))
    own.wait()
    dense_own.wait()
    for item in dense_copies:
        item.wait()
    for k in range(1, wide):

        @pl.when((me ^ k) < pieces)
        def _():
            for item in shared_copies(k):
                item.wait_send()

        @pl.when(me < pieces)
        def _():
            place = pl.ds(pl.multiple_of((me ^ k) * LANES, LANES), LANES)
            landed = (all_gate.at[place], all_up.at[place], all_down.at[:, place])
            for number, target in enumerate(landed):
                copy(W + k + (number + 1) * wide, target, target, twin).wait_recv()

    for item in started:
        item.wait_send()

    def other(chip, side=None):
        start = chip * count + (1 - core) * rows
        if side is None:
            return every.at[pl.ds(pl.multiple_of(start, rows), rows)]
        return every.at[pl.ds(pl.multiple_of(start + side * half, half), half)]

    for d in range(lines):
        if d > 0:
            place = other(me ^ (PLANE * d))
            copy(T + Z + d, place, place, twin).wait_recv()
        for base, flip, side in ((X, 1, None), (Y, 2, None), (XD, 3, 0), (YD, 3, 1)):
            place = other(me ^ flip ^ (PLANE * d), side)
            copy(T + base + d, place, place, twin).wait_recv()


def gather(wide, tokens, gate, up, down, dense):
    count, width = tokens.shape
    lines = wide // PLANE
    sems = 10 * lines + 4 * wide
    bf16 = jnp.bfloat16
    return pl.pallas_call(
        functools.partial(gather_kernel, wide),
        out_shape=(
            jax.ShapeDtypeStruct((wide * count, width), bf16),
            jax.ShapeDtypeStruct((wide * gate.shape[0], LANES), bf16),
            jax.ShapeDtypeStruct((wide * gate.shape[0], LANES), bf16),
            jax.ShapeDtypeStruct((LANES, wide * down.shape[1]), bf16),
            jax.ShapeDtypeStruct((wide, 8, count), jnp.float32),
        ),
        in_specs=[VMEM] * 5,
        out_specs=[VMEM] * 5,
        scratch_shapes=[
            pltpu.SemaphoreType.DMA((sems,)),
            pltpu.SemaphoreType.DMA((sems,)),
            pltpu.SemaphoreType.DMA((5,)),
        ],
        compiler_params=pltpu.CompilerParams(
            collective_id=0, has_side_effects=True, vmem_limit_bytes=60 << 20
        ),
    )(tokens, gate, up, down, dense)


def expert_kernel(group, slots, x, w, w_gate, w_up, w_down, s_gate, s_up, s_down, own, rows, slot_w, both):
    count = w.shape[2]
    f32, bf16 = jnp.float32, jnp.bfloat16
    hidden_count = w_gate.shape[1]
    lane_r = lax.broadcasted_iota(jnp.int32, (count, count), 0)
    lane_c = lax.broadcasted_iota(jnp.int32, (count, count), 1)
    upper = (lane_r <= lane_c).astype(f32).astype(bf16)
    slot = lax.broadcasted_iota(jnp.int32, (slots, count), 0).astype(f32)
    picks = []
    for b in range(group):
        weight = w[b]
        chosen = (weight > 0.0).astype(f32)
        rank = jnp.dot(chosen.astype(bf16), upper, preferred_element_type=f32)
        where = jnp.where(chosen > 0.0, rank - 1.0, -1.0)[0:1]
        pick = (jnp.broadcast_to(where, (slots, count)) == slot).astype(f32)
        picks.append(pick)
        place = pl.ds(b * slots, slots)
        slot_w[place] = jnp.sum(pick * weight[0:1], axis=1, keepdims=True)
        block = x[pl.ds(b * count, count)]
        rows[place] = jnp.dot(pick.astype(bf16), block, preferred_element_type=f32).astype(bf16)
    gate = jnp.dot(rows[...], w_gate[...], preferred_element_type=f32)
    up = jnp.dot(rows[...], w_up[...], preferred_element_type=f32)
    hidden = (jax.nn.silu(gate) * up * slot_w[...]).astype(bf16)
    for b in range(group):
        spread = jnp.dot(
            picks[b].T.astype(bf16),
            hidden[b * slots : (b + 1) * slots],
            preferred_element_type=f32,
        )
        both[pl.ds(b * count, count), :hidden_count] = spread.astype(bf16)
    gate = jnp.dot(x[...], s_gate[...], preferred_element_type=f32)
    up = jnp.dot(x[...], s_up[...], preferred_element_type=f32)
    shared = (jax.nn.silu(gate) * up).astype(bf16)
    width = own.shape[3]
    routed = both[...]
    for h in range(own.shape[0]):
        columns = slice(h * width, (h + 1) * width)
        part = jnp.dot(routed, w_down[:, columns], preferred_element_type=f32)
        part += jnp.dot(shared, s_down[:, columns], preferred_element_type=f32)
        own[h] = part.astype(bf16).reshape(group, count, width)


def expert(slots, every, weight, w_gate, w_up, w_down, s_gate, s_up, s_down, narrow):
    wide, _, count = weight.shape
    width = every.shape[1]
    group = 4
    whole = lambda a: pl.BlockSpec(a.shape, lambda i: (0, 0))
    return pl.pallas_call(
        functools.partial(expert_kernel, group, slots),
        grid=(wide // group,),
        out_shape=jax.ShapeDtypeStruct((narrow, wide, count, width // narrow), jnp.bfloat16),
        in_specs=[
            pl.BlockSpec((group * count, width), lambda i: (i, 0)),
            pl.BlockSpec((group, 8, count), lambda i: (i, 0, 0)),
            whole(w_gate),
            whole(w_up),
            whole(w_down),
            whole(s_gate),
            whole(s_up),
            whole(s_down),
        ],
        out_specs=pl.BlockSpec((narrow, group, count, width // narrow), lambda i: (0, i, 0, 0)),
        scratch_shapes=[
            pltpu.VMEM((group * slots, width), jnp.bfloat16),
            pltpu.VMEM((group * slots, 1), jnp.float32),
            pltpu.VMEM((group * count, w_gate.shape[1]), jnp.bfloat16),
        ],
        compiler_params=pltpu.CompilerParams(vmem_limit_bytes=60 << 20),
    )(every, weight, w_gate, w_up, w_down, s_gate, s_up, s_down)


def reduce_kernel(wide, part, out, twin_in, diag_in, side_in, line_in, send, recv, local, acc):
    me = lax.axis_index("wide")
    core = lax.axis_index("narrow")
    lines = wide // PLANE
    count = out.shape[0]
    half = count // 2
    x_peer, y_peer, twin = (me ^ 1, core), (me ^ 2, core), (me, 1 - core)
    zs = [(me ^ (PLANE * d), core) for d in range(1, lines)]
    greet([twin, x_peer, y_peer] + zs)
    T, XD, YD, X, Y, Z = 0, wide, wide + lines, wide + 2 * lines, wide + 3 * lines, wide + 4 * lines
    started = []

    def copy(number, source, target, device):
        return pltpu.make_async_remote_copy(
            src_ref=source,
            dst_ref=target,
            send_sem=send.at[number],
            recv_sem=recv.at[number],
            device_id=device,
            device_id_type=MESH,
        )

    def start(item):
        item.start()
        started.append(item)

    def arrive(number, place):
        copy(number, place, place, twin).wait_recv()

    step = 16

    def add(target, sources, first, total):
        def one(i, carry):
            at = pl.ds(pl.multiple_of(first + i * step, step), step)
            value = target[at].astype(jnp.float32)
            for source, shift in sources:
                value += source[pl.ds(pl.multiple_of(first + i * step - shift, step), step)].astype(
                    jnp.float32
                )
            target[at] = value.astype(jnp.bfloat16)
            return carry

        lax.fori_loop(0, total // step, one, 0)

    order = list(range(1, lines)) + [0]
    chips = [flip ^ (PLANE * d) for flip in (3, 2, 1, 0) for d in order]
    mine = []
    for k in chips:
        chip = me ^ k
        start(copy(T + k, part.at[1 - core, chip], twin_in.at[k], twin))
        item = pltpu.make_async_copy(part.at[core, chip], acc.at[k], local.at[k])
        item.start()
        mine.append(item)

    def fold(k):
        mine[chips.index(k)].wait()
        arrive(T + k, twin_in.at[k])
        add(acc.at[k], [(twin_in.at[k], 0)], 0, count)

    for d in order:
        k = 3 ^ (PLANE * d)
        fold(k)
        start(copy(XD + d, acc.at[k, pl.ds(0, half)], diag_in.at[0, d], x_peer))
        start(copy(YD + d, acc.at[k, pl.ds(half, half)], diag_in.at[1, d], y_peer))
    for d in order:
        fold(2 ^ (PLANE * d))
        fold(1 ^ (PLANE * d))
    for d in order:
        k = 2 ^ (PLANE * d)
        arrive(XD + d, diag_in.at[0, d])
        add(acc.at[k], [(diag_in.at[0, d], 0)], 0, half)
        start(copy(Y + d, acc.at[k], side_in.at[1, d], y_peer))
        k = 1 ^ (PLANE * d)
        arrive(YD + d, diag_in.at[1, d])
        add(acc.at[k], [(diag_in.at[1, d], half)], half, half)
        start(copy(X + d, acc.at[k], side_in.at[0, d], x_peer))
    for d in order:
        fold(PLANE * d)
    for d in order:
        k = PLANE * d
        arrive(X + d, side_in.at[0, d])
        arrive(Y + d, side_in.at[1, d])
        if d > 0:
            add(acc.at[k], [(side_in.at[0, d], 0), (side_in.at[1, d], 0)], 0, count)
            start(copy(Z + d, acc.at[k], line_in.at[d], (me ^ k, core)))
    for d in range(1, lines):
        arrive(Z + d, line_in.at[d])

    def last(i, carry):
        at = pl.ds(pl.multiple_of(i * step, step), step)
        value = acc[0, at].astype(jnp.float32)
        value += side_in[0, 0, at].astype(jnp.float32) + side_in[1, 0, at].astype(jnp.float32)
        for d in range(1, lines):
            value += line_in[d, at].astype(jnp.float32)
        out[at] = value.astype(jnp.bfloat16)
        return carry

    lax.fori_loop(0, count // step, last, 0)
    for item in started:
        item.wait_send()


def reduce(part):
    narrow, wide, count, width = part.shape
    lines = wide // PLANE
    sems = wide + 5 * lines
    bf16 = jnp.bfloat16
    return pl.pallas_call(
        functools.partial(reduce_kernel, wide),
        out_shape=jax.ShapeDtypeStruct((count, width), bf16),
        in_specs=[VMEM],
        out_specs=VMEM,
        scratch_shapes=[
            pltpu.VMEM((wide, count, width), bf16),
            pltpu.VMEM((2, lines, count // 2, width), bf16),
            pltpu.VMEM((2, lines, count, width), bf16),
            pltpu.VMEM((lines, count, width), bf16),
            pltpu.SemaphoreType.DMA((sems,)),
            pltpu.SemaphoreType.DMA((sems,)),
            pltpu.SemaphoreType.DMA((wide,)),
            pltpu.VMEM((wide, count, width), bf16),
        ],
        compiler_params=pltpu.CompilerParams(
            collective_id=1, has_side_effects=True, vmem_limit_bytes=60 << 20
        ),
    )(part)


def gather_body(
    tokens,
    expert_ids,
    gate_weights,
    shared_gate,
    shared_up,
    shared_down,
    expert_gate,
    expert_up,
    expert_down,
):
    tok_count, top_count = expert_ids.shape
    wide = lax.axis_size("wide")
    narrow = lax.axis_size("narrow")
    experts = wide * expert_gate.shape[0]
    capacity, _ = plan(tok_count, top_count, experts, wide)
    names = jnp.arange(experts, dtype=jnp.int32)
    match = expert_ids.T[None, :, :] == names[:, None, None]
    dense = jnp.sum(jnp.where(match, gate_weights.T[None, :, :], 0.0), axis=1)
    dense = jnp.broadcast_to(dense[:, None, :], (experts, 8, tok_count))
    every, s_gate, s_up, s_down, weight = gather(
        wide, tokens, shared_gate, shared_up, shared_down, dense
    )
    part = expert(
        capacity,
        every,
        weight,
        expert_gate[0],
        expert_up[0],
        expert_down[0],
        s_gate,
        s_up,
        s_down,
        narrow,
    )
    return reduce(part)


def solution(mesh):
    in_specs = (
        P("wide", None),
        P("wide", None),
        P("wide", None),
        P("wide", "narrow"),
        P("wide", "narrow"),
        P("narrow", "wide"),
        P("wide", None, "narrow"),
        P("wide", None, "narrow"),
        P("wide", "narrow", None),
    )
    out_specs = P("wide", "narrow")
    wide_count = mesh.shape["wide"]

    def body(*args):
        tok_count, top_count = args[1].shape
        gathers = plan(tok_count, top_count, wide_count * args[6].shape[0], wide_count)[1]
        return (gather_body if gathers else dispatch_body)(*args)

    return jax.shard_map(body, mesh=mesh, in_specs=in_specs, out_specs=out_specs, check_vma=False)
```

```python
import functools

import jax
import jax.numpy as jnp
from jax import lax
from jax.experimental import pallas as pl
from jax.experimental.pallas import tpu as pltpu
from jax.sharding import PartitionSpec as P


def expert_ffn(received, w_gate, w_up, w_down):
    senders, items, width = received.shape
    flat_rows = received.reshape(senders * items, width)
    gate_part = jnp.dot(flat_rows, w_gate, preferred_element_type=jnp.float32)
    up_part = jnp.dot(flat_rows, w_up, preferred_element_type=jnp.float32)
    hidden = (jax.nn.silu(gate_part) * up_part).astype(jnp.bfloat16)
    partial_value = jnp.dot(hidden, w_down, preferred_element_type=jnp.float32).astype(jnp.bfloat16)
    return partial_value.reshape(senders, items, w_down.shape[1])


def dispatch_body(
    tokens,
    expert_ids,
    gate_weights,
    shared_gate,
    shared_up,
    shared_down,
    expert_gate,
    expert_up,
    expert_down,
):
    tok_count, width = tokens.shape
    top_count = expert_ids.shape[1]
    experts = lax.axis_size("wide") * expert_gate.shape[0]
    capacity = min(tok_count, 4 * tok_count * top_count // (3 * experts))
    narrow_count = lax.axis_size("narrow")
    w_gate = expert_gate[0]
    w_up = expert_up[0]
    w_down = expert_down[0]
    pairs = tok_count * top_count
    flat_ids = expert_ids.reshape(pairs)
    onehot = (flat_ids[:, None] == jnp.arange(experts, dtype=jnp.int32)[None, :]).astype(jnp.int32)
    before = jnp.cumsum(onehot, axis=0) - onehot
    slot_pos = jnp.sum(before * onehot, axis=1)
    target_slot = flat_ids * capacity + slot_pos
    source = (
        jnp.full((experts * capacity,), -1, jnp.int32)
        .at[target_slot]
        .set(jnp.arange(pairs, dtype=jnp.int32))
    )
    filled = source >= 0
    token_of = jnp.where(filled, source // top_count, 0)
    outgoing = jnp.where(filled[:, None], tokens[token_of], jnp.zeros((), jnp.bfloat16))
    outgoing = outgoing.reshape(experts, capacity, width)
    quarter = capacity // narrow_count
    own_rows = lax.dynamic_slice_in_dim(outgoing, lax.axis_index("narrow") * quarter, quarter, 1)
    arrived = lax.all_to_all(own_rows, "wide", split_axis=0, concat_axis=0, tiled=True)
    joined = lax.all_gather(arrived, "narrow", axis=1, tiled=True)
    partial_value = expert_ffn(joined, w_gate, w_up, w_down)
    expert_out = (
        lax.psum_scatter(partial_value, "narrow", scatter_dimension=2, tiled=True)
        .astype(jnp.float32)
        .astype(jnp.bfloat16)
    )
    returned = lax.all_to_all(expert_out, "wide", split_axis=0, concat_axis=0, tiled=True)
    returned_rows = returned.reshape(experts * capacity, returned.shape[2])
    pair_rows = returned_rows[target_slot].astype(jnp.float32)
    weighted = gate_weights.reshape(pairs, 1) * pair_rows
    routed = jnp.sum(weighted.reshape(tok_count, top_count, returned.shape[2]), axis=1)
    gate_sum = jnp.dot(
        tokens,
        lax.all_gather(shared_gate, "wide", axis=0, tiled=True),
        preferred_element_type=jnp.float32,
    )
    up_sum = jnp.dot(
        tokens,
        lax.all_gather(shared_up, "wide", axis=0, tiled=True),
        preferred_element_type=jnp.float32,
    )
    shared_hidden = (jax.nn.silu(gate_sum) * up_sum).astype(jnp.bfloat16)
    shared_terms = jnp.dot(
        shared_hidden,
        lax.all_gather(shared_down, "wide", axis=1, tiled=True),
        preferred_element_type=jnp.float32,
    )
    shared = lax.psum_scatter(shared_terms, "narrow", scatter_dimension=1, tiled=True)
    return (shared + routed).astype(jnp.bfloat16)


MESH = pl.DeviceIdType.MESH
ANY = pl.BlockSpec(memory_space=pl.ANY)
VMEM = pl.BlockSpec(memory_space=pltpu.VMEM)
LANES = 128
PLANE = 4


def plan(tok_count, top_count, experts, wide_count):
    capacity = min(tok_count, 4 * tok_count * top_count // (3 * experts))
    return capacity, wide_count * tok_count <= 4 * experts * capacity


def greet(devices):
    barrier = pltpu.get_barrier_semaphore()
    for device in devices:
        pl.semaphore_signal(barrier, inc=1, device_id=device, device_id_type=MESH)
    pl.semaphore_wait(barrier, len(devices))


def fused_kernel(
    wide,
    slots,
    tok,
    gate,
    up,
    down,
    dense,
    w_gate_in,
    w_up_in,
    w_down_in,
    out,
    every,
    all_gate,
    all_up,
    all_down,
    weight,
    w_gate,
    w_up,
    w_down,
    rows,
    slot_w,
    both,
    other,
    acc,
    twin_in,
    diag_in,
    side_in,
    line_in,
    send,
    recv,
    local,
):
    f32, bf16 = jnp.float32, jnp.bfloat16
    me = lax.axis_index("wide")
    core = lax.axis_index("narrow")
    lines = wide // PLANE
    count = tok.shape[0]
    share = count // 2
    half = share // 2
    pieces = gate.shape[1] // LANES
    greet([(me ^ k, core) for k in range(1, wide)] + [(me, 1 - core)])
    x_peer, y_peer, twin = (me ^ 1, core), (me ^ 2, core), (me, 1 - core)
    started = []

    def pos(k):
        return (k % PLANE) * lines + k // PLANE

    def copy(number, source, target, device):
        return pltpu.make_async_remote_copy(
            src_ref=source,
            dst_ref=target,
            send_sem=send.at[number],
            recv_sem=recv.at[number],
            device_id=device,
            device_id_type=MESH,
        )

    def start(item):
        item.start()
        started.append(item)

    def landed(number, place):
        copy(number, place, place, twin).wait_recv()

    def region(k, side=None, of=core):
        begin = pos(k) * count + of * share
        if side is None:
            return every.at[pl.ds(pl.multiple_of(begin, share), share)]
        return every.at[pl.ds(pl.multiple_of(begin + side * half, half), half)]

    Z, X, Y, XD, YD, T = (lines * i for i in range(6))
    W = T + 5 * lines
    R = W + 4 * wide

    def arrive(number, place):
        landed(number, place)
        start(copy(T + number, place, place, twin))

    own = pltpu.make_async_copy(tok, every.at[pl.ds(0, count)], local.at[0])
    own.start()
    mine = tok.at[pl.ds(pl.multiple_of(core * share, share), share)]
    start(copy(X, mine, region(1), x_peer))
    start(copy(Y, mine, region(2), y_peer))
    for d in range(1, lines):
        start(copy(Z + d, mine, region(PLANE * d), (me ^ (PLANE * d), core)))
    for k in range(1, wide):
        start(copy(W + k, dense.at[me ^ k], weight.at[pos(k)], (me ^ k, core)))
    loads = [pltpu.make_async_copy(dense.at[me], weight.at[0], local.at[1])]
    for number, (source, target) in enumerate(
        ((w_gate_in, w_gate), (w_up_in, w_up), (w_down_in, w_down))
    ):
        loads.append(pltpu.make_async_copy(source, target, local.at[5 + number]))
    for item in loads:
        item.start()

    def shared_copies(k):
        part = pl.ds(pl.multiple_of((me ^ k) * LANES, LANES), LANES)
        place = pl.ds(pl.multiple_of(me * LANES, LANES), LANES)
        to = (me ^ k, core)
        return [
            copy(W + k + wide, gate.at[:, part], all_gate.at[place], to),
            copy(W + k + 2 * wide, up.at[:, part], all_up.at[place], to),
            copy(W + k + 3 * wide, down.at[part], all_down.at[:, place], to),
        ]

    def send_shared(ks):
        for k in ks:

            @pl.when((me ^ k) < pieces)
            def _():
                for item in shared_copies(k):
                    item.start()

    def line(d):
        arrive(Z + d, region(PLANE * d))
        start(copy(X + d, region(PLANE * d), region(PLANE * d ^ 1), x_peer))
        start(copy(Y + d, region(PLANE * d), region(PLANE * d ^ 2), y_peer))

    def beside(d):
        k = 1 ^ (PLANE * d)
        arrive(X + d, region(k))
        start(copy(YD + d, region(k, 1), region(k ^ 2, 1), y_peer))
        k = 2 ^ (PLANE * d)
        arrive(Y + d, region(k))
        start(copy(XD + d, region(k, 0), region(k ^ 1, 0), x_peer))

    send_shared(range(1, wide))
    beside(0)
    for d in range(1, lines):
        line(d)
        if d >= 2:
            beside(d - 1)

    @pl.when(me < pieces)
    def _():
        part = pl.ds(pl.multiple_of(me * LANES, LANES), LANES)
        items = [
            pltpu.make_async_copy(gate.at[:, part], all_gate.at[part], local.at[2]),
            pltpu.make_async_copy(up.at[:, part], all_up.at[part], local.at[3]),
            pltpu.make_async_copy(down.at[part], all_down.at[:, part], local.at[4]),
        ]
        for item in items:
            item.start()
        for item in items:
            item.wait()

    @pl.when(me >= pieces)
    def _():
        all_gate[...] = jnp.zeros_like(all_gate)
        all_up[...] = jnp.zeros_like(all_up)
        all_down[...] = jnp.zeros_like(all_down)

    beside(lines - 1)

    block = lines * count
    lane_r = lax.broadcasted_iota(jnp.int32, (count, count), 0)
    lane_c = lax.broadcasted_iota(jnp.int32, (count, count), 1)
    upper = (lane_r <= lane_c).astype(f32).astype(bf16)
    slot = lax.broadcasted_iota(jnp.int32, (slots, count), 0).astype(f32)

    def across(a, b):
        return lax.dot_general(a, b, (((1,), (1,)), ((), ())), preferred_element_type=f32)

    def routed_hidden(group):
        picks = []
        for b in range(lines):
            value = weight[group * lines + b]
            chosen = (value > 0.0).astype(f32)
            rank = jnp.dot(chosen.astype(bf16), upper, preferred_element_type=f32)
            where = jnp.where(chosen > 0.0, rank - 1.0, -1.0)[0:1]
            pick = (jnp.broadcast_to(where, (slots, count)) == slot).astype(f32)
            picks.append(pick)
            place = pl.ds(b * slots, slots)
            slot_w[place] = jnp.sum(pick * value[0:1], axis=1, keepdims=True)
            at = pl.ds(pl.multiple_of(group * block + b * count, count), count)
            rows[place] = jnp.dot(
                pick.astype(bf16), every[at], preferred_element_type=f32
            ).astype(bf16)
        gate_part = across(rows[...], w_gate[...])
        up_part = across(rows[...], w_up[...])
        hidden = (jax.nn.silu(gate_part) * up_part * slot_w[...]).astype(bf16)
        for b in range(lines):
            spread = jnp.dot(
                picks[b].T.astype(bf16),
                hidden[b * slots : (b + 1) * slots],
                preferred_element_type=f32,
            )
            at = pl.ds(pl.multiple_of(group * block + b * count, count), count)
            both[at] = spread.astype(bf16)

    width = out.shape[1]

    def finish(group):
        at = pl.ds(pl.multiple_of(group * block, block), block)
        gate_part = jnp.dot(every[at], all_gate[...], preferred_element_type=f32)
        up_part = jnp.dot(every[at], all_up[...], preferred_element_type=f32)
        shared = (jax.nn.silu(gate_part) * up_part).astype(bf16)
        for target, which in ((other, 1 - core), (acc, core)):
            columns = pl.ds(pl.multiple_of(which * width, width), width)
            part = jnp.dot(both[at], w_down[:, columns], preferred_element_type=f32)
            part += jnp.dot(shared, all_down[:, columns], preferred_element_type=f32)
            target[at] = part.astype(bf16)

    for k in range(1, wide):
        landed(W + k, weight.at[pos(k)])
    for item in loads:
        item.wait()
    own.wait()
    for d in range(lines):
        if d > 0:
            landed(T + Z + d, region(PLANE * d, None, 1 - core))
        landed(T + X + d, region(PLANE * d ^ 1, None, 1 - core))
        landed(T + Y + d, region(PLANE * d ^ 2, None, 1 - core))

    def early(group, carry):
        routed_hidden(group)
        return carry

    lax.fori_loop(0, 3, early, 0)
    for d in range(lines):
        arrive(XD + d, region(3 ^ (PLANE * d), 0))
        arrive(YD + d, region(3 ^ (PLANE * d), 1))
    for d in range(lines):
        landed(T + XD + d, region(3 ^ (PLANE * d), 0, 1 - core))
        landed(T + YD + d, region(3 ^ (PLANE * d), 1, 1 - core))
    routed_hidden(3)
    for k in range(1, wide):

        @pl.when(me < pieces)
        def _():
            place = pl.ds(pl.multiple_of((me ^ k) * LANES, LANES), LANES)
            places = (all_gate.at[place], all_up.at[place], all_down.at[:, place])
            for number, target in enumerate(places):
                landed(W + k + (number + 1) * wide, target)

    RT, RXD, RYD = R, R + wide, R + wide + lines
    RX, RY, RZ = RYD + lines, RYD + 2 * lines, RYD + 3 * lines
    step = 16

    def rows_of(ref, k, begin=0, size=count):
        return ref.at[pl.ds(pos(k) * count + begin, size)]

    def add(target, sources):
        def one(i, carry):
            at = pl.ds(pl.multiple_of(i * step, step), step)
            value = target[at].astype(f32)
            for source in sources:
                value += source[at].astype(f32)
            target[at] = value.astype(bf16)
            return carry

        lax.fori_loop(0, target.shape[0] // step, one, 0)

    def hand_over(flip):
        finish(flip)
        for d in range(lines):
            k = flip ^ (PLANE * d)
            start(copy(RT + k, rows_of(other, k), rows_of(twin_in, k), twin))

    def fold(k):
        landed(RT + k, rows_of(twin_in, k))
        add(rows_of(acc, k), [rows_of(twin_in, k)])

    order = list(range(1, lines)) + [0]
    tall = count // 2
    hand_over(3)
    for d in order:
        k = 3 ^ (PLANE * d)
        fold(k)
        start(copy(RXD + d, rows_of(acc, k, 0, tall), diag_in.at[0, d], x_peer))
        start(copy(RYD + d, rows_of(acc, k, tall, tall), diag_in.at[1, d], y_peer))
    hand_over(2)
    hand_over(1)
    for d in order:
        k = 2 ^ (PLANE * d)
        fold(k)
        landed(RXD + d, diag_in.at[0, d])
        add(rows_of(acc, k, 0, tall), [diag_in.at[0, d]])
        start(copy(RY + d, rows_of(acc, k), side_in.at[1, d], y_peer))
        k = 1 ^ (PLANE * d)
        fold(k)
        landed(RYD + d, diag_in.at[1, d])
        add(rows_of(acc, k, tall, tall), [diag_in.at[1, d]])
        start(copy(RX + d, rows_of(acc, k), side_in.at[0, d], x_peer))
    hand_over(0)
    for d in order:
        fold(PLANE * d)
    for d in order:
        k = PLANE * d
        landed(RX + d, side_in.at[0, d])
        landed(RY + d, side_in.at[1, d])
        if d > 0:
            add(rows_of(acc, k), [side_in.at[0, d], side_in.at[1, d]])
            start(copy(RZ + d, rows_of(acc, k), line_in.at[d], (me ^ k, core)))
    for d in range(1, lines):
        landed(RZ + d, line_in.at[d])

    def last(i, carry):
        at = pl.ds(pl.multiple_of(i * step, step), step)
        value = acc[at].astype(f32)
        value += side_in[0, 0, at].astype(f32) + side_in[1, 0, at].astype(f32)
        for d in range(1, lines):
            value += line_in[d, at].astype(f32)
        out[at] = value.astype(bf16)
        return carry

    lax.fori_loop(0, count // step, last, 0)
    for k in range(1, wide):

        @pl.when((me ^ k) < pieces)
        def _():
            for item in shared_copies(k):
                item.wait_send()

    for item in started:
        item.wait_send()


def fused(wide, narrow, slots, tokens, gate, up, down, dense, w_gate, w_up, w_down):
    count, width = tokens.shape
    part = width // narrow
    lines = wide // PLANE
    total = wide * count
    sems = 10 * lines + 4 * wide + wide + 5 * lines
    bf16, f32 = jnp.bfloat16, jnp.float32
    return pl.pallas_call(
        functools.partial(fused_kernel, wide, slots),
        out_shape=jax.ShapeDtypeStruct((count, part), bf16),
        in_specs=[VMEM] * 5 + [ANY] * 3,
        out_specs=VMEM,
        scratch_shapes=[
            pltpu.VMEM((total, width), bf16),
            pltpu.VMEM((wide * gate.shape[0], LANES), bf16),
            pltpu.VMEM((wide * gate.shape[0], LANES), bf16),
            pltpu.VMEM((LANES, wide * down.shape[1]), bf16),
            pltpu.VMEM((wide, 8, count), f32),
            pltpu.VMEM(w_gate.shape, bf16),
            pltpu.VMEM(w_up.shape, bf16),
            pltpu.VMEM(w_down.shape, bf16),
            pltpu.VMEM((lines * slots, width), bf16),
            pltpu.VMEM((lines * slots, 1), f32),
            pltpu.VMEM((total, w_gate.shape[0]), bf16),
            pltpu.VMEM((total, part), bf16),
            pltpu.VMEM((total, part), bf16),
            pltpu.VMEM((total, part), bf16),
            pltpu.VMEM((2, lines, count // 2, part), bf16),
            pltpu.VMEM((2, lines, count, part), bf16),
            pltpu.VMEM((lines, count, part), bf16),
            pltpu.SemaphoreType.DMA((sems,)),
            pltpu.SemaphoreType.DMA((sems,)),
            pltpu.SemaphoreType.DMA((8,)),
        ],
        compiler_params=pltpu.CompilerParams(
            collective_id=0, has_side_effects=True, vmem_limit_bytes=63 << 20
        ),
    )(tokens, gate, up, down, dense, w_gate, w_up, w_down)


def gather_body(
    tokens,
    expert_ids,
    gate_weights,
    shared_gate,
    shared_up,
    shared_down,
    expert_gate,
    expert_up,
    expert_down,
):
    tok_count, top_count = expert_ids.shape
    wide = lax.axis_size("wide")
    narrow = lax.axis_size("narrow")
    experts = wide * expert_gate.shape[0]
    capacity, _ = plan(tok_count, top_count, experts, wide)
    names = jnp.arange(experts, dtype=jnp.int32)
    match = expert_ids.T[None, :, :] == names[:, None, None]
    dense = jnp.sum(jnp.where(match, gate_weights.T[None, :, :], 0.0), axis=1)
    dense = jnp.broadcast_to(dense[:, None, :], (experts, 8, tok_count))
    return fused(
        wide,
        narrow,
        capacity,
        tokens,
        shared_gate,
        shared_up,
        shared_down,
        dense,
        expert_gate[0].T,
        expert_up[0].T,
        expert_down[0],
    )


def solution(mesh):
    in_specs = (
        P("wide", None),
        P("wide", None),
        P("wide", None),
        P("wide", "narrow"),
        P("wide", "narrow"),
        P("narrow", "wide"),
        P("wide", None, "narrow"),
        P("wide", None, "narrow"),
        P("wide", "narrow", None),
    )
    out_specs = P("wide", "narrow")
    wide_count = mesh.shape["wide"]

    def body(*args):
        tok_count, top_count = args[1].shape
        gathers = plan(tok_count, top_count, wide_count * args[6].shape[0], wide_count)[1]
        return (gather_body if gathers else dispatch_body)(*args)

    return jax.shard_map(body, mesh=mesh, in_specs=in_specs, out_specs=out_specs, check_vma=False)
```

```python
import functools

import jax
import jax.numpy as jnp
from jax import lax
from jax.experimental import pallas as pl
from jax.experimental.pallas import tpu as pltpu
from jax.sharding import PartitionSpec as P


def expert_ffn(received, w_gate, w_up, w_down):
    senders, items, width = received.shape
    flat_rows = received.reshape(senders * items, width)
    gate_part = jnp.dot(flat_rows, w_gate, preferred_element_type=jnp.float32)
    up_part = jnp.dot(flat_rows, w_up, preferred_element_type=jnp.float32)
    hidden = (jax.nn.silu(gate_part) * up_part).astype(jnp.bfloat16)
    partial_value = jnp.dot(hidden, w_down, preferred_element_type=jnp.float32).astype(jnp.bfloat16)
    return partial_value.reshape(senders, items, w_down.shape[1])


def dispatch_body(
    tokens,
    expert_ids,
    gate_weights,
    shared_gate,
    shared_up,
    shared_down,
    expert_gate,
    expert_up,
    expert_down,
):
    tok_count, width = tokens.shape
    top_count = expert_ids.shape[1]
    experts = lax.axis_size("wide") * expert_gate.shape[0]
    capacity = min(tok_count, 4 * tok_count * top_count // (3 * experts))
    narrow_count = lax.axis_size("narrow")
    w_gate = expert_gate[0]
    w_up = expert_up[0]
    w_down = expert_down[0]
    pairs = tok_count * top_count
    flat_ids = expert_ids.reshape(pairs)
    onehot = (flat_ids[:, None] == jnp.arange(experts, dtype=jnp.int32)[None, :]).astype(jnp.int32)
    before = jnp.cumsum(onehot, axis=0) - onehot
    slot_pos = jnp.sum(before * onehot, axis=1)
    target_slot = flat_ids * capacity + slot_pos
    source = (
        jnp.full((experts * capacity,), -1, jnp.int32)
        .at[target_slot]
        .set(jnp.arange(pairs, dtype=jnp.int32))
    )
    filled = source >= 0
    token_of = jnp.where(filled, source // top_count, 0)
    outgoing = jnp.where(filled[:, None], tokens[token_of], jnp.zeros((), jnp.bfloat16))
    outgoing = outgoing.reshape(experts, capacity, width)
    quarter = capacity // narrow_count
    own_rows = lax.dynamic_slice_in_dim(outgoing, lax.axis_index("narrow") * quarter, quarter, 1)
    arrived = lax.all_to_all(own_rows, "wide", split_axis=0, concat_axis=0, tiled=True)
    joined = lax.all_gather(arrived, "narrow", axis=1, tiled=True)
    partial_value = expert_ffn(joined, w_gate, w_up, w_down)
    expert_out = (
        lax.psum_scatter(partial_value, "narrow", scatter_dimension=2, tiled=True)
        .astype(jnp.float32)
        .astype(jnp.bfloat16)
    )
    returned = lax.all_to_all(expert_out, "wide", split_axis=0, concat_axis=0, tiled=True)
    returned_rows = returned.reshape(experts * capacity, returned.shape[2])
    pair_rows = returned_rows[target_slot].astype(jnp.float32)
    weighted = gate_weights.reshape(pairs, 1) * pair_rows
    routed = jnp.sum(weighted.reshape(tok_count, top_count, returned.shape[2]), axis=1)
    gate_sum = jnp.dot(
        tokens,
        lax.all_gather(shared_gate, "wide", axis=0, tiled=True),
        preferred_element_type=jnp.float32,
    )
    up_sum = jnp.dot(
        tokens,
        lax.all_gather(shared_up, "wide", axis=0, tiled=True),
        preferred_element_type=jnp.float32,
    )
    shared_hidden = (jax.nn.silu(gate_sum) * up_sum).astype(jnp.bfloat16)
    shared_terms = jnp.dot(
        shared_hidden,
        lax.all_gather(shared_down, "wide", axis=1, tiled=True),
        preferred_element_type=jnp.float32,
    )
    shared = lax.psum_scatter(shared_terms, "narrow", scatter_dimension=1, tiled=True)
    return (shared + routed).astype(jnp.bfloat16)


MESH = pl.DeviceIdType.MESH
ANY = pl.BlockSpec(memory_space=pl.ANY)
VMEM = pl.BlockSpec(memory_space=pltpu.VMEM)
LANES = 128
PLANE = 4


def plan(tok_count, top_count, experts, wide_count):
    capacity = min(tok_count, 4 * tok_count * top_count // (3 * experts))
    return capacity, wide_count * tok_count <= 4 * experts * capacity


def greet(devices):
    barrier = pltpu.get_barrier_semaphore()
    for device in devices:
        pl.semaphore_signal(barrier, inc=1, device_id=device, device_id_type=MESH)
    pl.semaphore_wait(barrier, len(devices))


def fused_kernel(
    wide,
    slots,
    tok,
    gate,
    up,
    down,
    dense,
    w_gate_in,
    w_up_in,
    w_down_in,
    out,
    every,
    all_gate,
    all_up,
    all_down,
    weight,
    w_gate,
    w_up,
    w_down,
    rows,
    slot_w,
    both,
    other,
    acc,
    twin_in,
    diag_in,
    side_in,
    line_in,
    send,
    recv,
    local,
):
    f32, bf16 = jnp.float32, jnp.bfloat16
    me = lax.axis_index("wide")
    core = lax.axis_index("narrow")
    lines = wide // PLANE
    count = tok.shape[0]
    share = count // 2
    half = share // 2
    pieces = gate.shape[1] // LANES
    greet([(me ^ k, core) for k in range(1, wide)] + [(me, 1 - core)])
    x_peer, y_peer, twin = (me ^ 1, core), (me ^ 2, core), (me, 1 - core)
    started = []

    def pos(k):
        return (k % PLANE) * lines + k // PLANE

    def copy(number, source, target, device):
        return pltpu.make_async_remote_copy(
            src_ref=source,
            dst_ref=target,
            send_sem=send.at[number],
            recv_sem=recv.at[number],
            device_id=device,
            device_id_type=MESH,
        )

    def start(item):
        item.start()
        started.append(item)

    def landed(number, place):
        copy(number, place, place, twin).wait_recv()

    def region(k, side=None, of=core):
        begin = pos(k) * count + of * share
        if side is None:
            return every.at[pl.ds(pl.multiple_of(begin, share), share)]
        return every.at[pl.ds(pl.multiple_of(begin + side * half, half), half)]

    Z, X, Y, XD, YD, T = (lines * i for i in range(6))
    W = T + 5 * lines
    R = W + 4 * wide

    def arrive(number, place):
        landed(number, place)
        start(copy(T + number, place, place, twin))

    own = pltpu.make_async_copy(tok, every.at[pl.ds(0, count)], local.at[0])
    own.start()
    mine = tok.at[pl.ds(pl.multiple_of(core * share, share), share)]
    start(copy(X, mine, region(1), x_peer))
    start(copy(Y, mine, region(2), y_peer))
    for d in range(1, lines):
        start(copy(Z + d, mine, region(PLANE * d), (me ^ (PLANE * d), core)))
    for k in range(1, wide):
        start(copy(W + k, dense.at[me ^ k], weight.at[pos(k)], (me ^ k, core)))
    loads = [pltpu.make_async_copy(dense.at[me], weight.at[0], local.at[1])]
    for number, (source, target) in enumerate(
        ((w_gate_in, w_gate), (w_up_in, w_up), (w_down_in, w_down))
    ):
        loads.append(pltpu.make_async_copy(source, target, local.at[5 + number]))
    for item in loads:
        item.start()

    def shared_copies(k):
        part = pl.ds(pl.multiple_of((me ^ k) * LANES, LANES), LANES)
        place = pl.ds(pl.multiple_of(me * LANES, LANES), LANES)
        to = (me ^ k, core)
        return [
            copy(W + k + wide, gate.at[:, part], all_gate.at[place], to),
            copy(W + k + 2 * wide, up.at[:, part], all_up.at[place], to),
            copy(W + k + 3 * wide, down.at[part], all_down.at[:, place], to),
        ]

    def send_shared(ks):
        for k in ks:

            @pl.when((me ^ k) < pieces)
            def _():
                for item in shared_copies(k):
                    item.start()

    def line(d):
        arrive(Z + d, region(PLANE * d))
        start(copy(X + d, region(PLANE * d), region(PLANE * d ^ 1), x_peer))
        start(copy(Y + d, region(PLANE * d), region(PLANE * d ^ 2), y_peer))

    def beside(d):
        k = 1 ^ (PLANE * d)
        arrive(X + d, region(k))
        start(copy(YD + d, region(k, 1), region(k ^ 2, 1), y_peer))
        k = 2 ^ (PLANE * d)
        arrive(Y + d, region(k))
        start(copy(XD + d, region(k, 0), region(k ^ 1, 0), x_peer))

    send_shared(range(1, wide))
    beside(0)
    for d in range(1, lines):
        line(d)
        if d >= 2:
            beside(d - 1)

    @pl.when(me < pieces)
    def _():
        part = pl.ds(pl.multiple_of(me * LANES, LANES), LANES)
        items = [
            pltpu.make_async_copy(gate.at[:, part], all_gate.at[part], local.at[2]),
            pltpu.make_async_copy(up.at[:, part], all_up.at[part], local.at[3]),
            pltpu.make_async_copy(down.at[part], all_down.at[:, part], local.at[4]),
        ]
        for item in items:
            item.start()
        for item in items:
            item.wait()

    @pl.when(me >= pieces)
    def _():
        all_gate[...] = jnp.zeros_like(all_gate)
        all_up[...] = jnp.zeros_like(all_up)
        all_down[...] = jnp.zeros_like(all_down)

    block = lines * count
    lane_r = lax.broadcasted_iota(jnp.int32, (count, count), 0)
    lane_c = lax.broadcasted_iota(jnp.int32, (count, count), 1)
    upper = (lane_r <= lane_c).astype(f32).astype(bf16)
    slot = lax.broadcasted_iota(jnp.int32, (slots, count), 0).astype(f32)

    def across(a, b):
        return lax.dot_general(a, b, (((1,), (1,)), ((), ())), preferred_element_type=f32)

    def routed_hidden(group):
        picks = []
        for b in range(lines):
            value = weight[group * lines + b]
            chosen = (value > 0.0).astype(f32)
            rank = jnp.dot(chosen.astype(bf16), upper, preferred_element_type=f32)
            where = jnp.where(chosen > 0.0, rank - 1.0, -1.0)[0:1]
            pick = (jnp.broadcast_to(where, (slots, count)) == slot).astype(f32)
            picks.append(pick)
            place = pl.ds(b * slots, slots)
            slot_w[place] = jnp.sum(pick * value[0:1], axis=1, keepdims=True)
            at = pl.ds(pl.multiple_of(group * block + b * count, count), count)
            rows[place] = jnp.dot(
                pick.astype(bf16), every[at], preferred_element_type=f32
            ).astype(bf16)
        gate_part = across(rows[...], w_gate[...])
        up_part = across(rows[...], w_up[...])
        hidden = (jax.nn.silu(gate_part) * up_part * slot_w[...]).astype(bf16)
        for b in range(lines):
            spread = jnp.dot(
                picks[b].T.astype(bf16),
                hidden[b * slots : (b + 1) * slots],
                preferred_element_type=f32,
            )
            at = pl.ds(pl.multiple_of(group * block + b * count, count), count)
            both[at] = spread.astype(bf16)

    width = out.shape[1]

    def finish(group):
        at = pl.ds(pl.multiple_of(group * block, block), block)
        gate_part = jnp.dot(every[at], all_gate[...], preferred_element_type=f32)
        up_part = jnp.dot(every[at], all_up[...], preferred_element_type=f32)
        shared = (jax.nn.silu(gate_part) * up_part).astype(bf16)
        for target, which in ((other, 1 - core), (acc, core)):
            columns = pl.ds(pl.multiple_of(which * width, width), width)
            part = jnp.dot(both[at], w_down[:, columns], preferred_element_type=f32)
            part += jnp.dot(shared, all_down[:, columns], preferred_element_type=f32)
            target[at] = part.astype(bf16)

    for k in range(1, wide):
        landed(W + k, weight.at[pos(k)])
    for item in loads:
        item.wait()
    own.wait()
    for d in range(1, lines):
        landed(T + Z + d, region(PLANE * d, None, 1 - core))
    routed_hidden(0)
    beside(lines - 1)
    for d in range(lines):
        landed(T + X + d, region(PLANE * d ^ 1, None, 1 - core))
        landed(T + Y + d, region(PLANE * d ^ 2, None, 1 - core))

    def early(group, carry):
        routed_hidden(group)
        return carry

    lax.fori_loop(1, 3, early, 0)
    for d in range(lines):
        arrive(XD + d, region(3 ^ (PLANE * d), 0))
        arrive(YD + d, region(3 ^ (PLANE * d), 1))
    for d in range(lines):
        landed(T + XD + d, region(3 ^ (PLANE * d), 0, 1 - core))
        landed(T + YD + d, region(3 ^ (PLANE * d), 1, 1 - core))
    routed_hidden(3)
    for k in range(1, wide):

        @pl.when(me < pieces)
        def _():
            place = pl.ds(pl.multiple_of((me ^ k) * LANES, LANES), LANES)
            places = (all_gate.at[place], all_up.at[place], all_down.at[:, place])
            for number, target in enumerate(places):
                landed(W + k + (number + 1) * wide, target)

    RT, RXD, RYD = R, R + wide, R + wide + lines
    RX, RY, RZ = RYD + lines, RYD + 2 * lines, RYD + 3 * lines
    step = 16

    def rows_of(ref, k, begin=0, size=count):
        return ref.at[pl.ds(pos(k) * count + begin, size)]

    def add(target, sources):
        def one(i, carry):
            at = pl.ds(pl.multiple_of(i * step, step), step)
            value = target[at].astype(f32)
            for source in sources:
                value += source[at].astype(f32)
            target[at] = value.astype(bf16)
            return carry

        lax.fori_loop(0, target.shape[0] // step, one, 0)

    def hand_over(flip):
        finish(flip)
        for d in range(lines):
            k = flip ^ (PLANE * d)
            start(copy(RT + k, rows_of(other, k), rows_of(twin_in, k), twin))

    def fold(k):
        landed(RT + k, rows_of(twin_in, k))
        add(rows_of(acc, k), [rows_of(twin_in, k)])

    order = list(range(lines - 1, 0, -1)) + [0]
    tall = count // 2
    hand_over(3)
    for d in order:
        k = 3 ^ (PLANE * d)
        fold(k)
        start(copy(RXD + d, rows_of(acc, k, 0, tall), diag_in.at[0, d], x_peer))
        start(copy(RYD + d, rows_of(acc, k, tall, tall), diag_in.at[1, d], y_peer))
    hand_over(2)
    hand_over(1)
    for d in order:
        k = 2 ^ (PLANE * d)
        fold(k)
        landed(RXD + d, diag_in.at[0, d])
        add(rows_of(acc, k, 0, tall), [diag_in.at[0, d]])
        start(copy(RY + d, rows_of(acc, k), side_in.at[1, d], y_peer))
        k = 1 ^ (PLANE * d)
        fold(k)
        landed(RYD + d, diag_in.at[1, d])
        add(rows_of(acc, k, tall, tall), [diag_in.at[1, d]])
        start(copy(RX + d, rows_of(acc, k), side_in.at[0, d], x_peer))
    hand_over(0)
    for d in order:
        fold(PLANE * d)
    for d in order:
        k = PLANE * d
        landed(RX + d, side_in.at[0, d])
        landed(RY + d, side_in.at[1, d])
        if d > 0:
            add(rows_of(acc, k), [side_in.at[0, d], side_in.at[1, d]])
            start(copy(RZ + d, rows_of(acc, k), line_in.at[d], (me ^ k, core)))
    for d in range(1, lines):
        landed(RZ + d, line_in.at[d])

    def last(i, carry):
        at = pl.ds(pl.multiple_of(i * step, step), step)
        value = acc[at].astype(f32)
        value += side_in[0, 0, at].astype(f32) + side_in[1, 0, at].astype(f32)
        for d in range(1, lines):
            value += line_in[d, at].astype(f32)
        out[at] = value.astype(bf16)
        return carry

    lax.fori_loop(0, count // step, last, 0)
    for k in range(1, wide):

        @pl.when((me ^ k) < pieces)
        def _():
            for item in shared_copies(k):
                item.wait_send()

    for item in started:
        item.wait_send()


def fused(wide, narrow, slots, tokens, gate, up, down, dense, w_gate, w_up, w_down):
    count, width = tokens.shape
    part = width // narrow
    lines = wide // PLANE
    total = wide * count
    sems = 10 * lines + 4 * wide + wide + 5 * lines
    bf16, f32 = jnp.bfloat16, jnp.float32
    return pl.pallas_call(
        functools.partial(fused_kernel, wide, slots),
        out_shape=jax.ShapeDtypeStruct((count, part), bf16),
        in_specs=[VMEM] * 5 + [ANY] * 3,
        out_specs=VMEM,
        scratch_shapes=[
            pltpu.VMEM((total, width), bf16),
            pltpu.VMEM((wide * gate.shape[0], LANES), bf16),
            pltpu.VMEM((wide * gate.shape[0], LANES), bf16),
            pltpu.VMEM((LANES, wide * down.shape[1]), bf16),
            pltpu.VMEM((wide, 8, count), f32),
            pltpu.VMEM(w_gate.shape, bf16),
            pltpu.VMEM(w_up.shape, bf16),
            pltpu.VMEM(w_down.shape, bf16),
            pltpu.VMEM((lines * slots, width), bf16),
            pltpu.VMEM((lines * slots, 1), f32),
            pltpu.VMEM((total, w_gate.shape[0]), bf16),
            pltpu.VMEM((total, part), bf16),
            pltpu.VMEM((total, part), bf16),
            pltpu.VMEM((total, part), bf16),
            pltpu.VMEM((2, lines, count // 2, part), bf16),
            pltpu.VMEM((2, lines, count, part), bf16),
            pltpu.VMEM((lines, count, part), bf16),
            pltpu.SemaphoreType.DMA((sems,)),
            pltpu.SemaphoreType.DMA((sems,)),
            pltpu.SemaphoreType.DMA((8,)),
        ],
        compiler_params=pltpu.CompilerParams(
            collective_id=0, has_side_effects=True, vmem_limit_bytes=63 << 20
        ),
    )(tokens, gate, up, down, dense, w_gate, w_up, w_down)


def gather_body(
    tokens,
    expert_ids,
    gate_weights,
    shared_gate,
    shared_up,
    shared_down,
    expert_gate,
    expert_up,
    expert_down,
):
    tok_count, top_count = expert_ids.shape
    wide = lax.axis_size("wide")
    narrow = lax.axis_size("narrow")
    experts = wide * expert_gate.shape[0]
    capacity, _ = plan(tok_count, top_count, experts, wide)
    names = jnp.arange(experts, dtype=jnp.int32)
    match = expert_ids.T[None, :, :] == names[:, None, None]
    dense = jnp.sum(jnp.where(match, gate_weights.T[None, :, :], 0.0), axis=1)
    dense = jnp.broadcast_to(dense[:, None, :], (experts, 8, tok_count))
    return fused(
        wide,
        narrow,
        capacity,
        tokens,
        shared_gate,
        shared_up,
        shared_down,
        dense,
        expert_gate[0].T,
        expert_up[0].T,
        expert_down[0],
    )


def solution(mesh):
    in_specs = (
        P("wide", None),
        P("wide", None),
        P("wide", None),
        P("wide", "narrow"),
        P("wide", "narrow"),
        P("narrow", "wide"),
        P("wide", None, "narrow"),
        P("wide", None, "narrow"),
        P("wide", "narrow", None),
    )
    out_specs = P("wide", "narrow")
    wide_count = mesh.shape["wide"]

    def body(*args):
        tok_count, top_count = args[1].shape
        gathers = plan(tok_count, top_count, wide_count * args[6].shape[0], wide_count)[1]
        return (gather_body if gathers else dispatch_body)(*args)

    return jax.shard_map(body, mesh=mesh, in_specs=in_specs, out_specs=out_specs, check_vma=False)
```
